32 devices in a mesh: bl: 8 (over y, x, core), bp: 4 (over z).
Axes of the slice: x: 2, y: 2, z: 4, core: 2. Of those that a mesh axis runs over, the one named last changes fastest.
Arguments:
- inverse_cov: float32 [8, 1024, 1024], P('bl', 'bp'), may hold values from -1 to 12, as said below
- channel_keep_mask: int32 [8, 1024], P('bl'), may hold values 0 or 1
- partner_ids: int32 [8, 2], P('bl'), may hold values from -1 to 7, as said below
- band_starts: int32 [2, 64], replicated, may hold values from 0 to 384
Outputs:
- fisher: float32 [2, 64, 64], P(None, 'bp', 'bl')
The draws below stay inside these ranges and needn't reach their ends.
Inputs may be any that keep to these rules, and one draw needn't show every extreme that they name: partner_ids[i, k] is -1 for an empty slot, else the index of a baseline whose group, its index // 1, lies 1 to 4 groups after the group of baseline i, counted cyclically over the 8 groups; in every draw some baseline has all 2 slots filled. Each inverse_cov[i] is symmetric.
All inputs are finite; a program needn't handle non-finite values. No bound on the sum of `channel_keep_mask` on one device may be relied on, other than what follows from the above.
Results may differ from the reference program's by a relative error of at most 0.0003.
Values sent between devices are 32-bit elements; how exact they have to be, the bound alone decides.
A program may use at most 128 MiB of HBM per device.

```python
from functools import partial
import jax
import jax.numpy as jnp
from jax import lax

CHANNEL_COUNT = 1024
PANEL = 512
BANDPOWER_COUNT = 64
WINDOW_LENGTH = 128
PAIRS_PER_SHARD = 1
ANTENNA_PAIRS = 8
COMPANION_SEATS = 2
GROUP_REACH = 4


def draw_inverse_cov(key, part):
    seed_sequence = jax.random.split(key, 5)
    rough_estimate = jax.random.uniform(seed_sequence[0], (ANTENNA_PAIRS, CHANNEL_COUNT, CHANNEL_COUNT), jnp.float32, -1.0, 1.0)
    coupled = (rough_estimate + jnp.swapaxes(rough_estimate, 1, 2)) * (0.5 / 32.0)
    identity = jnp.eye(CHANNEL_COUNT, dtype=jnp.float32)
    diagonal_entries = jax.random.uniform(seed_sequence[1], (ANTENNA_PAIRS, CHANNEL_COUNT), jnp.float32, 1.0, 2.0)
    channel_weighting = jax.random.uniform(seed_sequence[2], (ANTENNA_PAIRS, CHANNEL_COUNT), jnp.float32, 0.5, 1.5)
    correlation_length = jnp.exp(jax.random.uniform(seed_sequence[3], (ANTENNA_PAIRS,), jnp.float32, jnp.log(CHANNEL_COUNT / 4.0), jnp.log(CHANNEL_COUNT * 1.0)))
    signal_amplitude = jax.random.uniform(seed_sequence[4], (ANTENNA_PAIRS,), jnp.float32, 0.04, 0.1)
    channel_pos = jnp.arange(CHANNEL_COUNT, dtype=jnp.float32)
    spread = jnp.abs(channel_pos[:, None] - channel_pos[None, :])
    smooth = signal_amplitude[:, None, None] * channel_weighting[:, :, None] * channel_weighting[:, None, :] * jnp.exp(-spread[None, :, :] / correlation_length[:, None, None])
    alternating = 1.0 - 2.0 * (jnp.arange(CHANNEL_COUNT, dtype=jnp.int32) % 2).astype(jnp.float32)
    parity = 0.1 * alternating[:, None] * alternating[None, :]
    matrix = coupled * (1.0 - identity) + identity * diagonal_entries[:, :, None] + smooth + parity[None, :, :]
    return matrix


def draw_partner_ids(key, part):
    seed_sequence = jax.random.split(key, 6)
    antenna_pair_sets = ANTENNA_PAIRS // PAIRS_PER_SHARD
    antenna_pair_number = jnp.arange(ANTENNA_PAIRS, dtype=jnp.int32)
    rotation_team = antenna_pair_number // PAIRS_PER_SHARD
    turn_shift = jax.random.randint(seed_sequence[0], (), 0, GROUP_REACH, dtype=jnp.int32)
    phase_bit = jax.random.randint(seed_sequence[1], (), 0, 2, dtype=jnp.int32)
    heaviest_group = jax.random.randint(seed_sequence[2], (), 0, ANTENNA_PAIRS, dtype=jnp.int32)
    additional_step = jax.random.randint(seed_sequence[3], (ANTENNA_PAIRS, COMPANION_SEATS), 0, GROUP_REACH, dtype=jnp.int32)
    team_element = jax.random.randint(seed_sequence[4], (ANTENNA_PAIRS, COMPANION_SEATS), 0, PAIRS_PER_SHARD, dtype=jnp.int32)
    keep_probability = jax.random.randint(seed_sequence[5], (ANTENNA_PAIRS, COMPANION_SEATS), 0, 10, dtype=jnp.int32)
    slot_ids = jnp.arange(COMPANION_SEATS, dtype=jnp.int32)[None, :]
    first_hop = ((rotation_team + turn_shift) % GROUP_REACH)[:, None]
    number_of_hops = 1 + jnp.where(slot_ids == 0, first_hop, additional_step)
    steady = ((rotation_team + phase_bit * GROUP_REACH) // GROUP_REACH % 2 == 0)[:, None] & (slot_ids == 0)
    filled = steady | (keep_probability < 3) | (antenna_pair_number == heaviest_group)[:, None]
    companion_pair = (rotation_team[:, None] + number_of_hops) % antenna_pair_sets * PAIRS_PER_SHARD + team_element
    return jnp.where(filled, companion_pair, -1).astype(jnp.int32)


def touch_ends(result, stream_key, low, top_value):
    shape = result.shape
    spot = [jax.random.randint(jax.random.fold_in(stream_key, axis), (), 0, shape[axis]) for axis in range(len(shape))]
    result = result.at[tuple(spot)].set(low)
    longest = shape.index(max(shape))
    spot[longest] = (spot[longest] + 1) % shape[longest]
    return result.at[tuple(spot)].set(top_value)


def setup_inputs(seed: int = 0) -> dict:
    keys = jax.random.split(jax.random.key(seed), 5)
    inverse_cov = draw_inverse_cov(jax.random.fold_in(keys[4], 71), 0)
    channel_keep_mask = touch_ends((jax.random.randint(keys[1], (ANTENNA_PAIRS, CHANNEL_COUNT), 0, 5) < 4).astype(jnp.int32), jax.random.fold_in(keys[1], 1), 0, 1)
    partner_ids = draw_partner_ids(jax.random.fold_in(keys[4], 71), 0)
    band_starts = touch_ends(jax.random.randint(keys[3], (2, BANDPOWER_COUNT), 0, PANEL - WINDOW_LENGTH + 1), jax.random.fold_in(keys[3], 1), 0, PANEL - WINDOW_LENGTH).astype(jnp.int32)
    return dict(inverse_cov=inverse_cov, channel_keep_mask=channel_keep_mask, partner_ids=partner_ids, band_starts=band_starts)


highest = lax.Precision.HIGHEST


def kernel_stack(first_band, band_count, window):
    channel_pos = jnp.arange(window, dtype=jnp.float32)
    spread = jnp.abs(channel_pos[:, None] - channel_pos[None, :])
    band_ids = first_band + jnp.arange(band_count, dtype=jnp.int32)
    length = 1.0 + (band_ids % 4).astype(jnp.float32)
    return jnp.exp(-spread[None, :, :] / length[:, None, None])


def project(panel_block, starts, kernels):
    window = kernels.shape[1]
    window_rows = jax.vmap(lambda row_start: lax.dynamic_slice_in_dim(panel_block, row_start, window, 0))(starts)
    return jnp.einsum("apq,aqc->apc", kernels, window_rows, precision=highest, preferred_element_type=jnp.float32)


def column_windows(projected, starts, window):
    def one_matrix(matrix):
        return jax.vmap(lambda column_start: lax.dynamic_slice_in_dim(matrix, column_start, window, 1))(starts)
    return jax.vmap(one_matrix)(projected)


def baseline_panels(inverse_cov, channel_keep_mask, index):
    matrix = lax.dynamic_index_in_dim(inverse_cov, index, 0, keepdims=False)
    flag_marks = lax.dynamic_index_in_dim(channel_keep_mask, index, 0, keepdims=False).astype(jnp.float32)
    halves = []
    for half_index in range(2):
        lower = half_index * PANEL
        block_part = matrix[lower:lower + PANEL, lower:lower + PANEL]
        marks_half = flag_marks[lower:lower + PANEL]
        halves.append(block_part * marks_half[:, None] * marks_half[None, :])
    return halves


def pair_fisher(own_rows, partner_rows, starts):
    def one_band(inputs):
        partner_row, band_begin = inputs
        partner_windows = column_windows(partner_row[None], starts, WINDOW_LENGTH)[0]
        own_windows = column_windows(own_rows, band_begin[None], WINDOW_LENGTH)[:, 0]
        return jnp.einsum("bpq,bqp->b", partner_windows, own_windows, precision=highest, preferred_element_type=jnp.float32)
    return lax.map(one_band, (partner_rows, starts))


def slot_fisher(inverse_cov, channel_keep_mask, band_starts, kernels, own_rows, target):
    partner_halves = baseline_panels(inverse_cov, channel_keep_mask, target)
    results = []
    for half_index in range(2):
        partner_rows = project(partner_halves[half_index], band_starts[half_index], kernels)
        results.append(pair_fisher(own_rows[half_index], partner_rows, band_starts[half_index]))
    return jnp.stack(results)


def reference(inverse_cov, channel_keep_mask, partner_ids, band_starts):
    kernels = kernel_stack(0, BANDPOWER_COUNT, WINDOW_LENGTH)

    def accumulate_fisher(index, running_totals):
        own_halves = baseline_panels(inverse_cov, channel_keep_mask, index)
        own_rows = [project(own_halves[half_index], band_starts[half_index], kernels) for half_index in range(2)]
        for slot_index in range(COMPANION_SEATS):
            target = partner_ids[index, slot_index]
            safe_target = jnp.maximum(target, 0).astype(jnp.int32)
            running_totals = running_totals + lax.cond(target >= 0, partial(slot_fisher, inverse_cov, channel_keep_mask, band_starts, kernels, own_rows, safe_target), partial(jnp.zeros, (2, BANDPOWER_COUNT, BANDPOWER_COUNT), jnp.float32))
        return running_totals

    running_totals = lax.fori_loop(0, ANTENNA_PAIRS, accumulate_fisher, jnp.zeros((2, BANDPOWER_COUNT, BANDPOWER_COUNT), jnp.float32))
    return running_totals * (1.0 / (4 * ANTENNA_PAIRS * WINDOW_LENGTH))
```

```python
from functools import partial

import jax
import jax.numpy as jnp
from jax import lax
from jax.experimental import pallas as pl
from jax.experimental.pallas import tpu as pltpu
from jax.sharding import PartitionSpec as P

WINDOW_LENGTH = 128
KINDS = 4
CHUNKS = 4
MESH = pl.DeviceIdType.MESH
NT = (((1,), (1,)), ((), ()))
NN = (((1,), (0,)), ((), ()))


def split(value):
    high = value.astype(jnp.bfloat16)
    return high, (value - high.astype(jnp.float32)).astype(jnp.bfloat16)


def dot(left, right, dims):
    return lax.dot_general(left, right, dims, preferred_element_type=jnp.float32)


def dot3(left, right, dims):
    return dot(left[0], right[0], dims) + (dot(left[0], right[1], dims) + dot(left[1], right[0], dims))


def exact(left, right, dims):
    return lax.dot_general(
        left, right, dims, precision=lax.Precision.HIGHEST, preferred_element_type=jnp.float32
    )


def column_of(row, length, offset):
    shape = (length, row.shape[1])
    spot = lax.broadcasted_iota(jnp.int32, shape, 0) + offset == lax.broadcasted_iota(jnp.int32, shape, 1)
    return jnp.sum(jnp.where(spot, row, 0.0), axis=1, keepdims=True)


def kernel(
    sizes, cov_ref, mask_ref, partner_ref, starts_ref, out_ref,
    raw, panel, near, far, sib_own, sib_near, sib_far, toep, toep_low, grown, other,
    inside, ramp, edge, edge_own, sums, tiles, landed, share, shares,
    load_sem, sib_sem, turn_sem, far_sem, near_sem, sfar_sem, snear_sem, fin_send, fin_recv, row_send, row_recv,
):
    groups, owners, rows, width, bands = sizes
    window = WINDOW_LENGTH
    me, level = lax.axis_index("bl"), lax.axis_index("bp")
    per_half = width // rows
    half, first = level // per_half, pl.multiple_of(level % per_half * rows, rows)
    pair, core = me // 2, me % 2
    pairs = groups // 2
    sibling = pair * 2 + 1 - core
    beside = (pair + 1 - 2 * (pair % 2)) * 2 + core
    behind = (pair + pairs - 2) % pairs * 2 + core
    level_other = level // per_half * per_half + (per_half - 1 - level % per_half)
    tile_rows = bands // groups
    band_share = bands // owners
    step = rows // CHUNKS

    load = pltpu.make_async_copy(
        cov_ref.at[0, :, pl.ds(pl.multiple_of(half * width, width), width)], raw, load_sem.at[0]
    )
    load.start()
    barrier = pltpu.get_barrier_semaphore()
    for d in range(1, groups):
        pl.semaphore_signal(barrier, inc=1, device_id=((me + d) % groups, level), device_id_type=MESH)
    for d in range(1, owners):
        pl.semaphore_signal(barrier, inc=1, device_id=(me, (level + d) % owners), device_id_type=MESH)

    marks = mask_ref[:, pl.ds(pl.multiple_of(half * width, width), width)].astype(jnp.float32)
    row_marks = column_of(marks, rows, first)
    load.wait()
    panel[pl.ds(first, rows), :] = raw[...] * row_marks * marks
    pl.semaphore_wait(barrier, groups + owners - 2)

    def remote(source, target, sems, index, device):
        return pltpu.make_async_remote_copy(
            src_ref=source, dst_ref=target, send_sem=sems.at[0, index], recv_sem=sems.at[1, index],
            device_id=device, device_id_type=MESH,
        )

    def own_at(q):
        return panel.at[pl.ds(pl.multiple_of(first + q * step, step), step)]

    def part(ref, q):
        return ref.at[pl.ds(q * step, step)]

    to_far = [remote(own_at(q), part(far, q), far_sem, q, (behind, level)) for q in range(CHUNKS)]
    near_direct = [remote(own_at(q), part(near, q), near_sem, q, (beside, level)) for q in range(CHUNKS)]
    near_relay = [remote(part(far, q), part(near, q), near_sem, q, (beside, level)) for q in range(CHUNKS)]
    far_on = [remote(part(far, q), part(sib_far, q), sfar_sem, q, (sibling, level)) for q in range(CHUNKS)]
    near_on = [remote(part(near, q), part(sib_near, q), snear_sem, q, (sibling, level)) for q in range(CHUNKS)]
    own_rows = panel.at[pl.ds(first, rows)]
    to_sibling = remote(own_rows, sib_own, sib_sem, 0, (sibling, level))
    to_turn = remote(own_rows, own_rows, turn_sem, 0, (me, level_other))
    other_first = pl.multiple_of(width - rows - first, rows)
    turn_in = panel.at[pl.ds(other_first, rows)]
    from_turn = remote(turn_in, turn_in, turn_sem, 0, (me, level_other))

    odd = pair % 2 == 1
    for q in range(CHUNKS):
        to_far[q].start()

        @pl.when(odd)
        def _():
            near_direct[q].start()

    to_turn.start()
    to_sibling.start()

    def relay(q):
        to_far[q].wait_recv()

        @pl.when(jnp.logical_not(odd))
        def _():
            near_relay[q].start()

        far_on[q].start()

    def forward(q):
        near_direct[q].wait_recv()
        near_on[q].start()

    def fill(kind, carry):
        far_apart = jnp.abs(
            lax.broadcasted_iota(jnp.int32, (width, width), 0) - lax.broadcasted_iota(jnp.int32, (width, width), 1)
        ).astype(jnp.float32)
        length = 1.0 + lax.convert_element_type(kind, jnp.float32)
        high, low = split(jnp.exp(-far_apart / length))
        toep[kind] = high
        toep_low[kind] = low
        return carry

    lax.fori_loop(0, KINDS, fill, 0)

    start_row = starts_ref[pl.ds(half, 1), :].astype(jnp.float32)
    start = column_of(start_row, bands, 0)
    band_ids = lax.broadcasted_iota(jnp.int32, (bands, 1), 0)
    inverse_length = 1.0 / (1.0 + (band_ids % KINDS).astype(jnp.float32))
    channel = lax.broadcasted_iota(jnp.int32, (bands, width), 1).astype(jnp.float32)
    ahead = channel - start
    past = ahead - (window - 1)
    within = jnp.logical_and(ahead >= 0.0, past <= 0.0)
    inside[...] = jnp.where(within, 1.0, 0.0)
    ramp[0:bands, :] = jnp.where(within, jnp.exp(-jnp.abs(ahead) * inverse_length), 0.0)
    ramp[bands:, :] = jnp.where(within, jnp.exp(-jnp.abs(past) * inverse_length), 0.0)
    edge[0:bands, :] = jnp.where(ahead < 0.0, jnp.exp(-jnp.abs(ahead) * inverse_length), 0.0)
    edge[bands:, :] = jnp.where(past > 0.0, jnp.exp(-jnp.abs(past) * inverse_length), 0.0)

    relay(0)
    relay(1)
    from_turn.wait_recv()
    ramps, edges = split(ramp[...]), split(edge[...])
    whole = split(panel[...])
    edge_own[...] = dot3(edges, whole, NN)

    def grow(kind, carry):
        mine = pl.ds(first, rows)
        grown[kind] = dot3((toep[kind, mine, :], toep_low[kind, mine, :]), whole, NN)
        sums[kind] = jnp.zeros((rows, bands), jnp.float32)
        return carry

    lax.fori_loop(0, KINDS // 2, grow, 0)
    relay(2)
    lax.fori_loop(KINDS // 2, KINDS, grow, 0)
    relay(3)
    across = dot3(split(edge_own[...]), ramps, NT)
    for q in range(CHUNKS):
        forward(q)
    to_sibling.wait_recv()
    for q in range(CHUNKS):
        far_on[q].wait_recv()
        near_on[q].wait_recv()

    def weight(baseline):
        total = jnp.float32(0.0)
        for slot in range(partner_ref.shape[1]):
            total = total + jnp.where(partner_ref[0, slot] == baseline, jnp.float32(1.0), jnp.float32(0.0))
        return total

    pair_near, pair_far = (pair + 1) % pairs * 2, (pair + 2) % pairs * 2
    summed = (
        sib_own[...] * weight(sibling)
        + near[...] * weight(pair_near + core)
        + far[...] * weight(pair_far + core)
        + sib_near[...] * weight(pair_near + 1 - core)
        + sib_far[...] * weight(pair_far + 1 - core)
    )
    partners = split(summed)
    mine = pl.ds(first, rows)
    ramp_mine = split(ramp[:, mine])
    leak = dot3(partners, edges, NT)
    inner = dot3(ramp_mine, split(leak), NN)
    cross = inner * across
    total = cross[0:bands, 0:bands] + cross[0:bands, bands:] + cross[bands:, 0:bands] + cross[bands:, bands:]

    other[...] = jnp.zeros((bands, 2 * bands), jnp.float32)

    def spread(kind, carry):
        turned = dot3(partners, (toep[kind], toep_low[kind]), NN)
        own_kind = (lax.broadcasted_iota(jnp.int32, (bands, 1), 0) % KINDS == kind).astype(jnp.float32)
        window_kind = (inside[...] * own_kind).astype(jnp.bfloat16)
        for m in range(KINDS):
            high, low = split(grown[m] * turned)
            sums[m] = sums[m] + (dot(high, window_kind, NT) + dot(low, window_kind, NT))
        high, low = split(dot3(ramp_mine, split(turned), NN) * edge_own[...])
        other[...] = other[...] + (dot(window_kind, high, NT) + dot(window_kind, low, NT))
        return carry

    lax.fori_loop(0, KINDS, spread, 0)
    inside_mine = inside[:, mine].astype(jnp.bfloat16)
    for m in range(KINDS):
        reach = leak * dot3(split(grown[m]), ramps, NT)
        high, low = split(sums[m] - reach[:, 0:bands] - reach[:, bands:])
        found = dot(inside_mine, high, NN) + dot(inside_mine, low, NN)
        total = total + jnp.where(band_ids % KINDS == m, found, 0.0)
    eye = (
        lax.broadcasted_iota(jnp.int32, (bands, bands), 0) == lax.broadcasted_iota(jnp.int32, (bands, bands), 1)
    ).astype(jnp.float32)
    side = other[...]
    flipped = exact(eye, total, NT) - side[:, 0:bands] - side[:, bands:]
    flipped = flipped * (1.0 / (4 * groups * window))

    for g in range(groups):
        tiles[g] = flipped[g * tile_rows:(g + 1) * tile_rows, :]
    landed[pl.ds(me, 1)] = tiles[pl.ds(me, 1)]
    outgoing = []
    for d in range(1, groups):
        peer = (me + d) % groups
        copy = pltpu.make_async_remote_copy(
            src_ref=tiles.at[peer], dst_ref=landed.at[me], send_sem=fin_send.at[peer], recv_sem=fin_recv.at[me],
            device_id=(peer, level), device_id_type=MESH,
        )
        copy.start()
        outgoing.append(copy)
    for d in range(1, groups):
        peer = (me + d) % groups
        pltpu.make_async_remote_copy(
            src_ref=tiles.at[peer], dst_ref=landed.at[peer], send_sem=fin_send.at[peer], recv_sem=fin_recv.at[peer],
            device_id=(peer, level), device_id_type=MESH,
        ).wait_recv()
    mine_sum = landed[0]
    for g in range(1, groups):
        mine_sum = mine_sum + landed[g]
    share[...] = mine_sum
    shares[pl.ds(level, 1)] = mine_sum[None]
    for d in range(1, owners):
        peer = (level + d) % owners
        copy = pltpu.make_async_remote_copy(
            src_ref=share, dst_ref=shares.at[level], send_sem=row_send.at[peer], recv_sem=row_recv.at[level],
            device_id=(me, peer), device_id_type=MESH,
        )
        copy.start()
        outgoing.append(copy)
    for d in range(1, owners):
        peer = (level + d) % owners
        pltpu.make_async_remote_copy(
            src_ref=share, dst_ref=shares.at[peer], send_sem=row_send.at[peer], recv_sem=row_recv.at[peer],
            device_id=(me, peer), device_id_type=MESH,
        ).wait_recv()
    pick = (
        lax.broadcasted_iota(jnp.int32, (band_share, bands), 0) + level * band_share
        == lax.broadcasted_iota(jnp.int32, (band_share, bands), 1)
    ).astype(jnp.float32)
    for h in range(2):
        tile = shares[h * per_half]
        for k in range(1, per_half):
            tile = tile + shares[h * per_half + k]
        out_ref[h] = exact(pick, tile, NT)

    for copy in outgoing:
        copy.wait_send()
    for q in range(CHUNKS):
        to_far[q].wait_send()
        near_direct[q].wait_send()
        far_on[q].wait_send()
        near_on[q].wait_send()
    to_sibling.wait_send()
    to_turn.wait_send()


def solution(mesh):
    groups, owners = mesh.shape["bl"], mesh.shape["bp"]

    def body(inverse_cov, channel_keep_mask, partner_ids, band_starts):
        count, rows, channels = inverse_cov.shape
        width, bands = channels // 2, band_starts.shape[1]
        assert count == 1 and groups % 4 == 0 and width == 2 * rows
        f32, bf16 = jnp.float32, jnp.bfloat16
        block = pltpu.VMEM((rows, width), f32)
        tile_rows = bands // groups
        dma = pltpu.SemaphoreType.DMA
        vmem = pl.BlockSpec(memory_space=pltpu.VMEM)
        return pl.pallas_call(
            partial(kernel, (groups, owners, rows, width, bands)),
            name="fisher",
            out_shape=jax.ShapeDtypeStruct((2, bands // owners, tile_rows), f32),
            in_specs=[pl.BlockSpec(memory_space=pl.ANY), vmem, pl.BlockSpec(memory_space=pltpu.SMEM), vmem],
            out_specs=vmem,
            scratch_shapes=[
                block,
                pltpu.VMEM((width, width), f32),
                block, block, block, block, block,
                pltpu.VMEM((KINDS, width, width), bf16),
                pltpu.VMEM((KINDS, width, width), bf16),
                pltpu.VMEM((KINDS, rows, width), f32),
                pltpu.VMEM((bands, 2 * bands), f32),
                pltpu.VMEM((bands, width), f32),
                pltpu.VMEM((2 * bands, width), f32),
                pltpu.VMEM((2 * bands, width), f32),
                pltpu.VMEM((2 * bands, width), f32),
                pltpu.VMEM((KINDS, rows, bands), f32),
                pltpu.VMEM((groups, tile_rows, bands), f32),
                pltpu.VMEM((groups, tile_rows, bands), f32),
                pltpu.VMEM((tile_rows, bands), f32),
                pltpu.VMEM((owners, tile_rows, bands), f32),
                dma((1,)), dma((2, 1)), dma((2, 1)),
                dma((2, CHUNKS)), dma((2, CHUNKS)), dma((2, CHUNKS)), dma((2, CHUNKS)),
                dma((groups,)), dma((groups,)), dma((owners,)), dma((owners,)),
            ],
            compiler_params=pltpu.CompilerParams(
                collective_id=0, has_side_effects=True, vmem_limit_bytes=48 * 1024 * 1024
            ),
        )(inverse_cov, channel_keep_mask, partner_ids, band_starts)

    placed = (P("bl", "bp", None), P("bl", None), P("bl", None), P())
    return jax.shard_map(body, mesh=mesh, in_specs=placed, out_specs=P(None, "bp", "bl"), check_vma=False)
```

```python
from functools import partial

import jax
import jax.numpy as jnp
from jax import lax
from jax.experimental import pallas as pl
from jax.experimental.pallas import tpu as pltpu
from jax.sharding import PartitionSpec as P

WINDOW_LENGTH = 128
KINDS = 4
CHUNKS = 8
MESH = pl.DeviceIdType.MESH
NT = (((1,), (1,)), ((), ()))
NN = (((1,), (0,)), ((), ()))


def split(value):
    high = value.astype(jnp.bfloat16)
    return high, (value - high.astype(jnp.float32)).astype(jnp.bfloat16)


def dot(left, right, dims):
    return lax.dot_general(left, right, dims, preferred_element_type=jnp.float32)


def dot3(left, right, dims):
    return dot(left[0], right[0], dims) + (dot(left[0], right[1], dims) + dot(left[1], right[0], dims))


def exact(left, right, dims):
    return lax.dot_general(
        left, right, dims, precision=lax.Precision.HIGHEST, preferred_element_type=jnp.float32
    )


def column_of(row, length, offset):
    shape = (length, row.shape[1])
    spot = lax.broadcasted_iota(jnp.int32, shape, 0) + offset == lax.broadcasted_iota(jnp.int32, shape, 1)
    return jnp.sum(jnp.where(spot, row, 0.0), axis=1, keepdims=True)


def kernel(
    sizes, cov_ref, mask_ref, partner_ref, starts_ref, out_ref,
    raw, masks, partner_row, starts, panel, near, far, sib_own, sib_near, sib_far, toep, toep_low, grown, felt,
    windows, ramp, edge, edge_own, crossed, tiles, landed, share, shares,
    load_sem, sib_sem, turn_sem, far_sem, near_sem, sfar_sem, snear_sem, fin_send, fin_recv, row_send, row_recv,
):
    groups, owners, rows, width, bands = sizes
    window = WINDOW_LENGTH
    me, level = lax.axis_index("bl"), lax.axis_index("bp")
    per_half = width // rows
    half, first = level // per_half, pl.multiple_of(level % per_half * rows, rows)
    pair, core = me // 2, me % 2
    pairs = groups // 2
    sibling = pair * 2 + 1 - core
    beside = (pair + 1 - 2 * (pair % 2)) * 2 + core
    behind = (pair + pairs - 2) % pairs * 2 + core
    level_other = level // per_half * per_half + (per_half - 1 - level % per_half)
    tile_rows = bands // groups
    band_share = bands // owners
    step = rows // CHUNKS

    half_columns = pl.ds(pl.multiple_of(half * width, width), width)
    loads = [
        pltpu.make_async_copy(source, target, load_sem.at[index])
        for index, (source, target) in enumerate([
            (cov_ref.at[0, :, half_columns], raw),
            (mask_ref, masks),
            (starts_ref, starts),
            (partner_ref, partner_row),
        ])
    ]
    for load in loads:
        load.start()
    barrier = pltpu.get_barrier_semaphore()
    for d in range(1, groups):
        pl.semaphore_signal(barrier, inc=1, device_id=((me + d) % groups, level), device_id_type=MESH)
    for d in range(1, owners):
        pl.semaphore_signal(barrier, inc=1, device_id=(me, (level + d) % owners), device_id_type=MESH)
    for load in loads:
        load.wait()

    marks = masks[:, half_columns].astype(jnp.float32)
    row_marks = column_of(marks, rows, first)
    panel[pl.ds(first, rows), :] = raw[...] * row_marks * marks
    pl.semaphore_wait(barrier, groups + owners - 2)

    def remote(source, target, sems, index, device):
        return pltpu.make_async_remote_copy(
            src_ref=source, dst_ref=target, send_sem=sems.at[0, index], recv_sem=sems.at[1, index],
            device_id=device, device_id_type=MESH,
        )

    def own_at(q):
        return panel.at[pl.ds(pl.multiple_of(first + q * step, step), step)]

    def part(ref, q):
        return ref.at[pl.ds(q * step, step)]

    to_far = [remote(own_at(q), part(far, q), far_sem, q, (behind, level)) for q in range(CHUNKS)]
    near_direct = [remote(own_at(q), part(near, q), near_sem, q, (beside, level)) for q in range(CHUNKS)]
    near_relay = [remote(part(far, q), part(near, q), near_sem, q, (beside, level)) for q in range(CHUNKS)]
    far_on = [remote(part(far, q), part(sib_far, q), sfar_sem, q, (sibling, level)) for q in range(CHUNKS)]
    near_on = [remote(part(near, q), part(sib_near, q), snear_sem, q, (sibling, level)) for q in range(CHUNKS)]
    own_rows = panel.at[pl.ds(first, rows)]
    to_sibling = remote(own_rows, sib_own, sib_sem, 0, (sibling, level))
    to_turn = remote(own_rows, own_rows, turn_sem, 0, (me, level_other))
    turn_in = panel.at[pl.ds(pl.multiple_of(width - rows - first, rows), rows)]
    from_turn = remote(turn_in, turn_in, turn_sem, 0, (me, level_other))

    odd = pair % 2 == 1
    for q in range(CHUNKS):
        to_far[q].start()

        @pl.when(odd)
        def _():
            near_direct[q].start()

    to_turn.start()
    to_sibling.start()

    def relay(q):
        to_far[q].wait_recv()

        @pl.when(jnp.logical_not(odd))
        def _():
            near_relay[q].start()

        far_on[q].start()

    def forward(q):
        near_direct[q].wait_recv()
        near_on[q].start()

    far_apart = jnp.abs(
        lax.broadcasted_iota(jnp.int32, (rows, rows), 0) - lax.broadcasted_iota(jnp.int32, (rows, rows), 1)
    ).astype(jnp.float32)
    for kind in range(KINDS):
        toep[kind], toep_low[kind] = split(jnp.exp(far_apart * (-1.0 / (1 + kind))))
    toeplitz = [(toep[kind], toep_low[kind]) for kind in range(KINDS)]

    start = column_of(starts[pl.ds(half, 1), :].astype(jnp.float32), bands, 0)
    band_ids = lax.broadcasted_iota(jnp.int32, (bands, 1), 0)
    inverse_length = 1.0 / (1.0 + (band_ids % KINDS).astype(jnp.float32))
    channel = lax.broadcasted_iota(jnp.int32, (bands, width), 1).astype(jnp.float32)
    ahead = channel - start
    past = ahead - (window - 1)
    within = jnp.logical_and(ahead >= 0.0, past <= 0.0)
    for kind in range(KINDS):
        windows[kind] = jnp.where(jnp.logical_and(within, band_ids % KINDS == kind), 1.0, 0.0).astype(jnp.bfloat16)
    windows[KINDS] = jnp.where(within, 1.0, 0.0).astype(jnp.bfloat16)
    rise, fall = jnp.exp(-jnp.abs(ahead) * inverse_length), jnp.exp(-jnp.abs(past) * inverse_length)
    ramp[0:bands, :] = jnp.where(within, rise, 0.0)
    ramp[bands:, :] = jnp.where(within, fall, 0.0)
    edge[0:bands, :] = jnp.where(ahead < 0.0, rise, 0.0)
    edge[bands:2 * bands, :] = jnp.where(past > 0.0, fall, 0.0)
    carry_ids = lax.broadcasted_iota(jnp.int32, (2 * KINDS, 1), 0)
    carry_length = 1.0 / (1.0 + (carry_ids % KINDS).astype(jnp.float32))
    carry_channel = lax.broadcasted_iota(jnp.int32, (2 * KINDS, width), 1).astype(jnp.float32) - rows
    upper = carry_ids < KINDS
    carry_gap = jnp.where(upper, carry_channel, -1.0 - carry_channel)
    edge[2 * bands:, :] = jnp.where(carry_gap >= 0.0, jnp.exp(-jnp.abs(carry_gap) * carry_length), 0.0)

    mine = pl.ds(first, rows)
    own_split = split(panel[mine, :])
    relay(0)
    for kind in range(KINDS):
        grown[kind] = dot3(toeplitz[kind], own_split, NN)
    relay(1)
    relay(2)
    from_turn.wait_recv()
    edges = split(edge[...])
    edge_own[...] = dot3(edges, split(panel[...]), NN)
    relay(3)
    ramps = split(ramp[...])
    place = lax.broadcasted_iota(jnp.int32, (rows, 1), 0)
    reach_in = jnp.where(first == 0, rows - place, place + 1).astype(jnp.float32)
    for kind in range(KINDS):
        carry = jnp.where(
            first == 0,
            edge_own[2 * bands + kind:2 * bands + kind + 1, :],
            edge_own[2 * bands + KINDS + kind:2 * bands + KINDS + kind + 1, :],
        )
        grown[kind] = grown[kind] + jnp.exp(reach_in * (-1.0 / (1 + kind))) * carry
        felt[kind] = dot3(split(grown[kind]), ramps, NT)
        if kind == 1:
            relay(4)
    own_edges = edge_own[0:2 * bands, :]
    across = dot3(split(own_edges), ramps, NT)
    relay(5)
    middle = CHUNKS // 2
    for q in range(middle):
        forward(q)
    to_sibling.wait_recv()

    def weight(baseline):
        return jnp.sum(jnp.where(partner_row[...] == baseline, 1.0, 0.0), axis=1, keepdims=True)

    pair_near, pair_far = (pair + 1) % pairs * 2, (pair + 2) % pairs * 2
    weights = [
        (sib_own, weight(sibling)), (near, weight(pair_near + core)), (far, weight(pair_far + core)),
        (sib_near, weight(pair_near + 1 - core)), (sib_far, weight(pair_far + 1 - core)),
    ]
    lane = lax.broadcasted_iota(jnp.int32, (1, rows), 1)

    def join(part_index, total, chores):
        span = rows // 2
        low_row = part_index * span
        for q in range(part_index * middle, (part_index + 1) * middle):
            far_on[q].wait_recv()
            near_on[q].wait_recv()
        here = slice(low_row, low_row + span)
        summed = sum(ref[here, :] * factor for ref, factor in weights)
        partners = split(summed)
        columns = pl.ds(pl.multiple_of(first + low_row, span), span)
        ramp_here = split(ramp[:, columns])
        leak = dot3(partners, edges, NT)
        leak_bands = leak[:, 0:2 * bands]
        inner = dot3(ramp_here, split(leak_bands), NN)
        sums = jnp.zeros((KINDS * span, bands), jnp.float32)
        for kind in range(KINDS):
            if kind < len(chores):
                chores[kind]()
            left = dot3((partners[0][:, 0:rows], partners[1][:, 0:rows]), toeplitz[kind], NN)
            left = left + leak[:, 2 * bands + kind:2 * bands + kind + 1] * jnp.exp(
                (rows - lane).astype(jnp.float32) * (-1.0 / (1 + kind)))
            right = dot3((partners[0][:, rows:], partners[1][:, rows:]), toeplitz[kind], NN)
            right = right + leak[:, 2 * bands + KINDS + kind:2 * bands + KINDS + kind + 1] * jnp.exp(
                (lane + 1).astype(jnp.float32) * (-1.0 / (1 + kind)))
            turned = jnp.concatenate([left, right], axis=1)
            pieces = [split(grown[m, here, :] * turned) for m in range(KINDS)]
            stacked = jnp.concatenate([p[0] for p in pieces] + [p[1] for p in pieces], axis=0)
            boxed = dot(stacked, windows[kind], NT)
            sums = sums + (boxed[0:KINDS * span] + boxed[KINDS * span:])
            found = dot3(ramp_here, split(turned), NN)
            crossed[kind] = found if part_index == 0 else crossed[kind] + found
        inside_here = windows[KINDS, :, columns]
        for m in range(KINDS):
            reach = leak_bands * felt[m, here, :]
            high, low = split(sums[m * span:(m + 1) * span] - reach[:, 0:bands] - reach[:, bands:])
            total = total + jnp.where(
                band_ids % KINDS == m, dot(inside_here, high, NN) + dot(inside_here, low, NN), 0.0)
        return inner, total

    inner_0, total = join(0, jnp.zeros((bands, bands), jnp.float32), [
        lambda: relay(6), lambda: relay(7), lambda: forward(4), lambda: forward(5)])
    for q in range(6, CHUNKS):
        forward(q)
    inner_1, total = join(1, total, [])
    cross = (inner_0 + inner_1) * across
    total = total + cross[0:bands, 0:bands] + cross[0:bands, bands:] + cross[bands:, 0:bands] + cross[bands:, bands:]
    side = jnp.zeros((bands, 2 * bands), jnp.float32)
    for kind in range(KINDS):
        high, low = split(crossed[kind] * own_edges)
        side = side + (dot(windows[kind], high, NT) + dot(windows[kind], low, NT))
    eye = (
        lax.broadcasted_iota(jnp.int32, (bands, bands), 0) == lax.broadcasted_iota(jnp.int32, (bands, bands), 1)
    ).astype(jnp.float32)
    flipped = exact(eye, total, NT) - side[:, 0:bands] - side[:, bands:]
    flipped = flipped * (1.0 / (4 * groups * window))

    for g in range(groups):
        tiles[g] = flipped[g * tile_rows:(g + 1) * tile_rows, :]
    landed[pl.ds(me, 1)] = tiles[pl.ds(me, 1)]
    outgoing = []
    for d in range(1, groups):
        peer = (me + d) % groups
        copy = pltpu.make_async_remote_copy(
            src_ref=tiles.at[peer], dst_ref=landed.at[me], send_sem=fin_send.at[peer], recv_sem=fin_recv.at[me],
            device_id=(peer, level), device_id_type=MESH,
        )
        copy.start()
        outgoing.append(copy)
    for d in range(1, groups):
        peer = (me + d) % groups
        pltpu.make_async_remote_copy(
            src_ref=tiles.at[peer], dst_ref=landed.at[peer], send_sem=fin_send.at[peer], recv_sem=fin_recv.at[peer],
            device_id=(peer, level), device_id_type=MESH,
        ).wait_recv()
    mine_sum = landed[0]
    for g in range(1, groups):
        mine_sum = mine_sum + landed[g]
    share[...] = mine_sum
    shares[pl.ds(level, 1)] = mine_sum[None]
    for d in range(1, owners):
        peer = (level + d) % owners
        copy = pltpu.make_async_remote_copy(
            src_ref=share, dst_ref=shares.at[level], send_sem=row_send.at[peer], recv_sem=row_recv.at[level],
            device_id=(me, peer), device_id_type=MESH,
        )
        copy.start()
        outgoing.append(copy)
    for d in range(1, owners):
        peer = (level + d) % owners
        pltpu.make_async_remote_copy(
            src_ref=share, dst_ref=shares.at[peer], send_sem=row_send.at[peer], recv_sem=row_recv.at[peer],
            device_id=(me, peer), device_id_type=MESH,
        ).wait_recv()
    pick = (
        lax.broadcasted_iota(jnp.int32, (band_share, bands), 0) + level * band_share
        == lax.broadcasted_iota(jnp.int32, (band_share, bands), 1)
    ).astype(jnp.float32)
    for h in range(2):
        tile = shares[h * per_half]
        for k in range(1, per_half):
            tile = tile + shares[h * per_half + k]
        out_ref[h] = exact(tile, pick, NT)

    for copy in outgoing:
        copy.wait_send()
    for q in range(CHUNKS):
        to_far[q].wait_send()
        near_direct[q].wait_send()
        far_on[q].wait_send()
        near_on[q].wait_send()
    to_sibling.wait_send()
    to_turn.wait_send()


def solution(mesh):
    groups, owners = mesh.shape["bl"], mesh.shape["bp"]

    def body(inverse_cov, channel_keep_mask, partner_ids, band_starts):
        count, rows, channels = inverse_cov.shape
        width, bands = channels // 2, band_starts.shape[1]
        assert count == 1 and groups % 4 == 0 and width == 2 * rows
        f32, bf16 = jnp.float32, jnp.bfloat16
        block = pltpu.VMEM((rows, width), f32)
        tile_rows = bands // groups
        dma = pltpu.SemaphoreType.DMA
        vmem = pl.BlockSpec(memory_space=pltpu.VMEM)
        found = pl.pallas_call(
            partial(kernel, (groups, owners, rows, width, bands)),
            name="fisher",
            out_shape=jax.ShapeDtypeStruct((2, tile_rows, bands // owners), f32),
            in_specs=[pl.BlockSpec(memory_space=pltpu.HBM)] * 4,
            out_specs=vmem,
            scratch_shapes=[
                block,
                pltpu.VMEM(channel_keep_mask.shape, jnp.int32),
                pltpu.VMEM(partner_ids.shape, jnp.int32),
                pltpu.VMEM(band_starts.shape, jnp.int32),
                pltpu.VMEM((width, width), f32),
                block, block, block, block, block,
                pltpu.VMEM((KINDS, rows, rows), bf16),
                pltpu.VMEM((KINDS, rows, rows), bf16),
                pltpu.VMEM((KINDS, rows, width), f32),
                pltpu.VMEM((KINDS, rows, 2 * bands), f32),
                pltpu.VMEM((KINDS + 1, bands, width), bf16),
                pltpu.VMEM((2 * bands, width), f32),
                pltpu.VMEM((2 * bands + 2 * KINDS, width), f32),
                pltpu.VMEM((2 * bands + 2 * KINDS, width), f32),
                pltpu.VMEM((KINDS, 2 * bands, width), f32),
                pltpu.VMEM((groups, tile_rows, bands), f32),
                pltpu.VMEM((groups, tile_rows, bands), f32),
                pltpu.VMEM((tile_rows, bands), f32),
                pltpu.VMEM((owners, tile_rows, bands), f32),
                dma((4,)), dma((2, 1)), dma((2, 1)),
                dma((2, CHUNKS)), dma((2, CHUNKS)), dma((2, CHUNKS)), dma((2, CHUNKS)),
                dma((groups,)), dma((groups,)), dma((owners,)), dma((owners,)),
            ],
            compiler_params=pltpu.CompilerParams(
                collective_id=0, has_side_effects=True, vmem_limit_bytes=67043328
            ),
        )(inverse_cov, channel_keep_mask, partner_ids, band_starts)
        return jnp.swapaxes(found, 1, 2)

    placed = (P("bl", "bp", None), P("bl", None), P("bl", None), P())
    return jax.shard_map(body, mesh=mesh, in_specs=placed, out_specs=P(None, "bp", "bl"), check_vma=False)
```

```python
from functools import partial

import jax
import jax.numpy as jnp
from jax import lax
from jax.experimental import pallas as pl
from jax.experimental.pallas import tpu as pltpu
from jax.sharding import PartitionSpec as P

WINDOW_LENGTH = 128
KINDS = 4
CHUNKS = 8
MESH = pl.DeviceIdType.MESH
NT = (((1,), (1,)), ((), ()))
NN = (((1,), (0,)), ((), ()))


def split(value):
    high = value.astype(jnp.bfloat16)
    return high, (value - high.astype(jnp.float32)).astype(jnp.bfloat16)


def dot(left, right, dims):
    return lax.dot_general(left, right, dims, preferred_element_type=jnp.float32)


def dot3(left, right, dims):
    return dot(left[0], right[0], dims) + (dot(left[0], right[1], dims) + dot(left[1], right[0], dims))


def exact(left, right, dims):
    return lax.dot_general(
        left, right, dims, precision=lax.Precision.HIGHEST, preferred_element_type=jnp.float32
    )


def column_of(row, length, offset):
    shape = (length, row.shape[1])
    spot = lax.broadcasted_iota(jnp.int32, shape, 0) + offset == lax.broadcasted_iota(jnp.int32, shape, 1)
    return jnp.sum(jnp.where(spot, row, 0.0), axis=1, keepdims=True)


def kernel(
    sizes, cov_ref, mask_ref, partner_ref, starts_ref, out_ref,
    raw, masks, partner_row, starts, panel, turn, near, far, sib_own, sib_near, sib_far, toep, toep_low, grown, felt,
    windows, ramp, edge, edge_own, crossed, tiles, landed, share, shares,
    load_sem, sib_sem, turn_sem, far_sem, near_sem, sfar_sem, snear_sem, fin_send, fin_recv, row_send, row_recv,
):
    groups, owners, rows, width, bands = sizes
    window = WINDOW_LENGTH
    me, level = lax.axis_index("bl"), lax.axis_index("bp")
    per_half = width // rows
    half, first = level // per_half, pl.multiple_of(level % per_half * rows, rows)
    pair, core = me // 2, me % 2
    pairs = groups // 2
    sibling = pair * 2 + 1 - core
    beside = (pair + 1 - 2 * (pair % 2)) * 2 + core
    behind = (pair + pairs - 2) % pairs * 2 + core
    level_other = level // per_half * per_half + (per_half - 1 - level % per_half)
    tile_rows = bands // groups
    band_share = bands // owners
    step = rows // CHUNKS

    half_columns = pl.ds(pl.multiple_of(half * width, width), width)
    loads = [
        pltpu.make_async_copy(source, target, load_sem.at[index])
        for index, (source, target) in enumerate([
            (cov_ref.at[0, :, half_columns], raw),
            (mask_ref, masks),
            (starts_ref, starts),
            (partner_ref, partner_row),
        ])
    ]
    for load in loads:
        load.start()
    barrier = pltpu.get_barrier_semaphore()
    for d in range(1, groups):
        pl.semaphore_signal(barrier, inc=1, device_id=((me + d) % groups, level), device_id_type=MESH)
    for d in range(1, owners):
        pl.semaphore_signal(barrier, inc=1, device_id=(me, (level + d) % owners), device_id_type=MESH)
    for load in loads:
        load.wait()

    marks = masks[:, half_columns].astype(jnp.float32)
    row_marks = column_of(marks, rows, first)
    panel[...] = raw[...] * row_marks * marks
    pl.semaphore_wait(barrier, groups + owners - 2)

    def remote(source, target, sems, index, device):
        return pltpu.make_async_remote_copy(
            src_ref=source, dst_ref=target, send_sem=sems.at[0, index], recv_sem=sems.at[1, index],
            device_id=device, device_id_type=MESH,
        )

    def own_at(q):
        return panel.at[pl.ds(q * step, step)]

    def part(ref, q):
        return ref.at[pl.ds(q * step, step)]

    to_far = [remote(own_at(q), part(far, q), far_sem, q, (behind, level)) for q in range(CHUNKS)]
    near_direct = [remote(own_at(q), part(near, q), near_sem, q, (beside, level)) for q in range(CHUNKS)]
    near_relay = [remote(part(far, q), part(near, q), near_sem, q, (beside, level)) for q in range(CHUNKS)]
    far_on = [remote(part(far, q), part(sib_far, q), sfar_sem, q, (sibling, level)) for q in range(CHUNKS)]
    near_on = [remote(part(near, q), part(sib_near, q), snear_sem, q, (sibling, level)) for q in range(CHUNKS)]
    mine = pl.ds(first, rows)
    theirs = pl.ds(pl.multiple_of(width - rows - first, rows), rows)
    to_sibling = remote(panel, sib_own, sib_sem, 0, (sibling, level))
    to_turn = remote(panel.at[:, mine], turn, turn_sem, 0, (me, level_other))

    odd = pair % 2 == 1
    for q in range(CHUNKS):
        to_far[q].start()

        @pl.when(odd)
        def _():
            near_direct[q].start()

    to_turn.start()
    to_sibling.start()

    def relay(q):
        to_far[q].wait_recv()

        @pl.when(jnp.logical_not(odd))
        def _():
            near_relay[q].start()

        far_on[q].start()

    def forward(q):
        near_direct[q].wait_recv()
        near_on[q].start()

    far_apart = jnp.abs(
        lax.broadcasted_iota(jnp.int32, (rows, rows), 0) - lax.broadcasted_iota(jnp.int32, (rows, rows), 1)
    ).astype(jnp.float32)
    for kind in range(KINDS):
        toep[kind], toep_low[kind] = split(jnp.exp(far_apart * (-1.0 / (1 + kind))))
    toeplitz = [(toep[kind], toep_low[kind]) for kind in range(KINDS)]

    start = column_of(starts[pl.ds(half, 1), :].astype(jnp.float32), bands, 0)
    band_ids = lax.broadcasted_iota(jnp.int32, (bands, 1), 0)
    inverse_length = 1.0 / (1.0 + (band_ids % KINDS).astype(jnp.float32))
    channel = lax.broadcasted_iota(jnp.int32, (bands, width), 1).astype(jnp.float32)
    ahead = channel - start
    past = ahead - (window - 1)
    within = jnp.logical_and(ahead >= 0.0, past <= 0.0)
    for kind in range(KINDS):
        windows[kind] = jnp.where(jnp.logical_and(within, band_ids % KINDS == kind), 1.0, 0.0).astype(jnp.bfloat16)
    windows[KINDS] = jnp.where(within, 1.0, 0.0).astype(jnp.bfloat16)
    rise, fall = jnp.exp(-jnp.abs(ahead) * inverse_length), jnp.exp(-jnp.abs(past) * inverse_length)
    ramp[0:bands, :] = jnp.where(within, rise, 0.0)
    ramp[bands:, :] = jnp.where(within, fall, 0.0)
    edge[0:bands, :] = jnp.where(ahead < 0.0, rise, 0.0)
    edge[bands:2 * bands, :] = jnp.where(past > 0.0, fall, 0.0)
    carry_ids = lax.broadcasted_iota(jnp.int32, (2 * KINDS, 1), 0)
    carry_length = 1.0 / (1.0 + (carry_ids % KINDS).astype(jnp.float32))
    carry_channel = lax.broadcasted_iota(jnp.int32, (2 * KINDS, width), 1).astype(jnp.float32) - rows
    upper = carry_ids < KINDS
    carry_gap = jnp.where(upper, carry_channel, -1.0 - carry_channel)
    edge[2 * bands:, :] = jnp.where(carry_gap >= 0.0, jnp.exp(-jnp.abs(carry_gap) * carry_length), 0.0)

    own_split = split(panel[...])
    relay(0)
    for kind in range(KINDS):
        grown[kind] = dot3(toeplitz[kind], own_split, NN)
    relay(1)
    edges = split(edge[...])
    edges_mine, edges_theirs = split(edge[:, mine]), split(edge[:, theirs])
    square, aside = split(panel[:, mine]), split(panel[:, theirs])
    edge_own[:, mine] = dot3(edges_mine, square, NN) + dot3(edges_theirs, aside, NT)
    relay(2)
    edge_own[:, theirs] = dot3(edges_mine, aside, NN)
    relay(3)
    to_turn.wait_recv()
    edge_own[:, theirs] = edge_own[:, theirs] + dot3(edges_theirs, split(turn[...]), NN)
    ramps = split(ramp[...])
    place = lax.broadcasted_iota(jnp.int32, (rows, 1), 0)
    reach_in = jnp.where(first == 0, rows - place, place + 1).astype(jnp.float32)
    for kind in range(KINDS):
        carry = jnp.where(
            first == 0,
            edge_own[2 * bands + kind:2 * bands + kind + 1, :],
            edge_own[2 * bands + KINDS + kind:2 * bands + KINDS + kind + 1, :],
        )
        grown[kind] = grown[kind] + jnp.exp(reach_in * (-1.0 / (1 + kind))) * carry
        felt[kind] = dot3(split(grown[kind]), ramps, NT)
        if kind == 1:
            relay(4)
    own_edges = edge_own[0:2 * bands, :]
    across = dot3(split(own_edges), ramps, NT)
    relay(5)
    middle = CHUNKS // 2
    for q in range(middle):
        forward(q)
    to_sibling.wait_recv()

    def weight(baseline):
        return jnp.sum(jnp.where(partner_row[...] == baseline, 1.0, 0.0), axis=1, keepdims=True)

    pair_near, pair_far = (pair + 1) % pairs * 2, (pair + 2) % pairs * 2
    weights = [
        (sib_own, weight(sibling)), (near, weight(pair_near + core)), (far, weight(pair_far + core)),
        (sib_near, weight(pair_near + 1 - core)), (sib_far, weight(pair_far + 1 - core)),
    ]
    lane = lax.broadcasted_iota(jnp.int32, (1, rows), 1)

    def join(part_index, total, chores):
        span = rows // 2
        low_row = part_index * span
        for q in range(part_index * middle, (part_index + 1) * middle):
            far_on[q].wait_recv()
            near_on[q].wait_recv()
        here = slice(low_row, low_row + span)
        summed = sum(ref[here, :] * factor for ref, factor in weights)
        partners = split(summed)
        columns = pl.ds(pl.multiple_of(first + low_row, span), span)
        ramp_here = split(ramp[:, columns])
        leak = dot3(partners, edges, NT)
        leak_bands = leak[:, 0:2 * bands]
        inner = dot3(ramp_here, split(leak_bands), NN)
        sums = jnp.zeros((KINDS * span, bands), jnp.float32)
        for kind in range(KINDS):
            if kind < len(chores):
                chores[kind]()
            left = dot3((partners[0][:, 0:rows], partners[1][:, 0:rows]), toeplitz[kind], NN)
            left = left + leak[:, 2 * bands + kind:2 * bands + kind + 1] * jnp.exp(
                (rows - lane).astype(jnp.float32) * (-1.0 / (1 + kind)))
            right = dot3((partners[0][:, rows:], partners[1][:, rows:]), toeplitz[kind], NN)
            right = right + leak[:, 2 * bands + KINDS + kind:2 * bands + KINDS + kind + 1] * jnp.exp(
                (lane + 1).astype(jnp.float32) * (-1.0 / (1 + kind)))
            turned = jnp.concatenate([left, right], axis=1)
            pieces = [split(grown[m, here, :] * turned) for m in range(KINDS)]
            stacked = jnp.concatenate([p[0] for p in pieces] + [p[1] for p in pieces], axis=0)
            boxed = dot(stacked, windows[kind], NT)
            sums = sums + (boxed[0:KINDS * span] + boxed[KINDS * span:])
            found = dot3(ramp_here, split(turned), NN)
            crossed[kind] = found if part_index == 0 else crossed[kind] + found
        inside_here = windows[KINDS, :, columns]
        for m in range(KINDS):
            reach = leak_bands * felt[m, here, :]
            high, low = split(sums[m * span:(m + 1) * span] - reach[:, 0:bands] - reach[:, bands:])
            total = total + jnp.where(
                band_ids % KINDS == m, dot(inside_here, high, NN) + dot(inside_here, low, NN), 0.0)
        return inner, total

    inner_0, total = join(0, jnp.zeros((bands, bands), jnp.float32), [
        lambda: relay(6), lambda: relay(7), lambda: forward(4), lambda: forward(5)])
    for q in range(6, CHUNKS):
        forward(q)
    inner_1, total = join(1, total, [])
    cross = (inner_0 + inner_1) * across
    total = total + cross[0:bands, 0:bands] + cross[0:bands, bands:] + cross[bands:, 0:bands] + cross[bands:, bands:]
    side = jnp.zeros((bands, 2 * bands), jnp.float32)
    for kind in range(KINDS):
        high, low = split(crossed[kind] * own_edges)
        side = side + (dot(windows[kind], high, NT) + dot(windows[kind], low, NT))
    eye = (
        lax.broadcasted_iota(jnp.int32, (bands, bands), 0) == lax.broadcasted_iota(jnp.int32, (bands, bands), 1)
    ).astype(jnp.float32)
    flipped = exact(eye, total, NT) - side[:, 0:bands] - side[:, bands:]
    flipped = flipped * (1.0 / (4 * groups * window))

    for g in range(groups):
        tiles[g] = flipped[g * tile_rows:(g + 1) * tile_rows, :]
    landed[pl.ds(me, 1)] = tiles[pl.ds(me, 1)]
    outgoing = []
    for d in range(1, groups):
        peer = (me + d) % groups
        copy = pltpu.make_async_remote_copy(
            src_ref=tiles.at[peer], dst_ref=landed.at[me], send_sem=fin_send.at[peer], recv_sem=fin_recv.at[me],
            device_id=(peer, level), device_id_type=MESH,
        )
        copy.start()
        outgoing.append(copy)
    for d in range(1, groups):
        peer = (me + d) % groups
        pltpu.make_async_remote_copy(
            src_ref=tiles.at[peer], dst_ref=landed.at[peer], send_sem=fin_send.at[peer], recv_sem=fin_recv.at[peer],
            device_id=(peer, level), device_id_type=MESH,
        ).wait_recv()
    mine_sum = landed[0]
    for g in range(1, groups):
        mine_sum = mine_sum + landed[g]
    share[...] = mine_sum
    shares[pl.ds(level, 1)] = mine_sum[None]
    for d in range(1, owners):
        peer = (level + d) % owners
        copy = pltpu.make_async_remote_copy(
            src_ref=share, dst_ref=shares.at[level], send_sem=row_send.at[peer], recv_sem=row_recv.at[level],
            device_id=(me, peer), device_id_type=MESH,
        )
        copy.start()
        outgoing.append(copy)
    for d in range(1, owners):
        peer = (level + d) % owners
        pltpu.make_async_remote_copy(
            src_ref=share, dst_ref=shares.at[peer], send_sem=row_send.at[peer], recv_sem=row_recv.at[peer],
            device_id=(me, peer), device_id_type=MESH,
        ).wait_recv()
    pick = (
        lax.broadcasted_iota(jnp.int32, (band_share, bands), 0) + level * band_share
        == lax.broadcasted_iota(jnp.int32, (band_share, bands), 1)
    ).astype(jnp.float32)
    for h in range(2):
        tile = shares[h * per_half]
        for k in range(1, per_half):
            tile = tile + shares[h * per_half + k]
        out_ref[h] = exact(tile, pick, NT)

    for copy in outgoing:
        copy.wait_send()
    for q in range(CHUNKS):
        to_far[q].wait_send()
        near_direct[q].wait_send()
        far_on[q].wait_send()
        near_on[q].wait_send()
    to_sibling.wait_send()
    to_turn.wait_send()


def solution(mesh):
    groups, owners = mesh.shape["bl"], mesh.shape["bp"]

    def body(inverse_cov, channel_keep_mask, partner_ids, band_starts):
        count, rows, channels = inverse_cov.shape
        width, bands = channels // 2, band_starts.shape[1]
        assert count == 1 and groups % 4 == 0 and width == 2 * rows
        f32, bf16 = jnp.float32, jnp.bfloat16
        block = pltpu.VMEM((rows, width), f32)
        tile_rows = bands // groups
        dma = pltpu.SemaphoreType.DMA
        vmem = pl.BlockSpec(memory_space=pltpu.VMEM)
        found = pl.pallas_call(
            partial(kernel, (groups, owners, rows, width, bands)),
            name="fisher",
            out_shape=jax.ShapeDtypeStruct((2, tile_rows, bands // owners), f32),
            in_specs=[pl.BlockSpec(memory_space=pltpu.HBM)] * 4,
            out_specs=vmem,
            scratch_shapes=[
                block,
                pltpu.VMEM(channel_keep_mask.shape, jnp.int32),
                pltpu.VMEM(partner_ids.shape, jnp.int32),
                pltpu.VMEM(band_starts.shape, jnp.int32),
                block,
                pltpu.VMEM((rows, rows), f32),
                block, block, block, block, block,
                pltpu.VMEM((KINDS, rows, rows), bf16),
                pltpu.VMEM((KINDS, rows, rows), bf16),
                pltpu.VMEM((KINDS, rows, width), f32),
                pltpu.VMEM((KINDS, rows, 2 * bands), f32),
                pltpu.VMEM((KINDS + 1, bands, width), bf16),
                pltpu.VMEM((2 * bands, width), f32),
                pltpu.VMEM((2 * bands + 2 * KINDS, width), f32),
                pltpu.VMEM((2 * bands + 2 * KINDS, width), f32),
                pltpu.VMEM((KINDS, 2 * bands, width), f32),
                pltpu.VMEM((groups, tile_rows, bands), f32),
                pltpu.VMEM((groups, tile_rows, bands), f32),
                pltpu.VMEM((tile_rows, bands), f32),
                pltpu.VMEM((owners, tile_rows, bands), f32),
                dma((4,)), dma((2, 1)), dma((2, 1)),
                dma((2, CHUNKS)), dma((2, CHUNKS)), dma((2, CHUNKS)), dma((2, CHUNKS)),
                dma((groups,)), dma((groups,)), dma((owners,)), dma((owners,)),
            ],
            compiler_params=pltpu.CompilerParams(
                collective_id=0, has_side_effects=True, vmem_limit_bytes=67043328
            ),
        )(inverse_cov, channel_keep_mask, partner_ids, band_starts)
        return jnp.swapaxes(found, 1, 2)

    placed = (P("bl", "bp", None), P("bl", None), P("bl", None), P())
    return jax.shard_map(body, mesh=mesh, in_specs=placed, out_specs=P(None, "bp", "bl"), check_vma=False)
```

```python
from functools import partial

import jax
import jax.numpy as jnp
from jax import lax
from jax.experimental import pallas as pl
from jax.experimental.pallas import tpu as pltpu
from jax.sharding import PartitionSpec as P

WINDOW_LENGTH = 128
KINDS = 4
CHUNKS = 8
MESH = pl.DeviceIdType.MESH
NT = (((1,), (1,)), ((), ()))
NN = (((1,), (0,)), ((), ()))


def split(value):
    high = value.astype(jnp.bfloat16)
    return high, (value - high.astype(jnp.float32)).astype(jnp.bfloat16)


def dot(left, right, dims):
    return lax.dot_general(left, right, dims, preferred_element_type=jnp.float32)


def dot3(left, right, dims):
    return dot(left[0], right[0], dims) + (dot(left[0], right[1], dims) + dot(left[1], right[0], dims))


def exact(left, right, dims):
    return lax.dot_general(
        left, right, dims, precision=lax.Precision.HIGHEST, preferred_element_type=jnp.float32
    )


def column_of(row, length, offset):
    shape = (length, row.shape[1])
    spot = lax.broadcasted_iota(jnp.int32, shape, 0) + offset == lax.broadcasted_iota(jnp.int32, shape, 1)
    return jnp.sum(jnp.where(spot, row, 0.0), axis=1, keepdims=True)


def kernel(
    sizes, cov_ref, mask_ref, partner_ref, starts_ref, out_ref,
    raw, masks, partner_row, starts, panel, turn, near, far, sib_own, sib_near, sib_far, toep, toep_low, grown, felt,
    windows, ramp, edge, edge_own, crossed, tiles, landed,
    load_sem, sib_sem, turn_sem, far_sem, near_sem, sfar_sem, snear_sem, fin_send, fin_recv, ready,
):
    groups, owners, rows, width, bands = sizes
    window = WINDOW_LENGTH
    me, level = lax.axis_index("bl"), lax.axis_index("bp")
    per_half = width // rows
    half, first = level // per_half, pl.multiple_of(level % per_half * rows, rows)
    pair, core = me // 2, me % 2
    pairs = groups // 2
    sibling = pair * 2 + 1 - core
    beside = (pair + 1 - 2 * (pair % 2)) * 2 + core
    behind = (pair + pairs - 2) % pairs * 2 + core
    level_other = level // per_half * per_half + (per_half - 1 - level % per_half)
    tile_rows = bands // groups
    band_share = bands // owners
    step = rows // CHUNKS

    half_columns = pl.ds(pl.multiple_of(half * width, width), width)
    loads = [
        pltpu.make_async_copy(source, target, load_sem.at[index])
        for index, (source, target) in enumerate([
            (cov_ref.at[0, :, half_columns], raw),
            (mask_ref, masks),
            (starts_ref, starts),
            (partner_ref, partner_row),
        ])
    ]
    for load in loads:
        load.start()
    barrier = pltpu.get_barrier_semaphore()
    for d in range(1, groups):
        pl.semaphore_signal(barrier, inc=1, device_id=((me + d) % groups, level), device_id_type=MESH)
    for d in range(1, owners):
        pl.semaphore_signal(barrier, inc=1, device_id=(me, (level + d) % owners), device_id_type=MESH)
    for load in loads:
        load.wait()

    marks = masks[:, half_columns].astype(jnp.float32)
    row_marks = column_of(marks, rows, first)
    panel[...] = raw[...] * row_marks * marks
    pl.semaphore_wait(barrier, groups + owners - 2)

    def remote(source, target, sems, index, device):
        return pltpu.make_async_remote_copy(
            src_ref=source, dst_ref=target, send_sem=sems.at[0, index], recv_sem=sems.at[1, index],
            device_id=device, device_id_type=MESH,
        )

    def own_at(q):
        return panel.at[pl.ds(q * step, step)]

    def part(ref, q):
        return ref.at[pl.ds(q * step, step)]

    to_far = [remote(own_at(q), part(far, q), far_sem, q, (behind, level)) for q in range(CHUNKS)]
    near_direct = [remote(own_at(q), part(near, q), near_sem, q, (beside, level)) for q in range(CHUNKS)]
    near_relay = [remote(part(far, q), part(near, q), near_sem, q, (beside, level)) for q in range(CHUNKS)]
    far_on = [remote(part(far, q), part(sib_far, q), sfar_sem, q, (sibling, level)) for q in range(CHUNKS)]
    near_on = [remote(part(near, q), part(sib_near, q), snear_sem, q, (sibling, level)) for q in range(CHUNKS)]
    mine = pl.ds(first, rows)
    theirs = pl.ds(pl.multiple_of(width - rows - first, rows), rows)
    to_sibling = remote(panel, sib_own, sib_sem, 0, (sibling, level))
    to_turn = remote(panel.at[:, mine], turn, turn_sem, 0, (me, level_other))

    odd = pair % 2 == 1
    for q in range(CHUNKS):
        to_far[q].start()

        @pl.when(odd)
        def _():
            near_direct[q].start()

    to_turn.start()
    to_sibling.start()
    for d in range(1, groups):
        pl.semaphore_signal(ready, inc=1, device_id=((me + d) % groups, level), device_id_type=MESH)

    def relay(q):
        to_far[q].wait_recv()

        @pl.when(jnp.logical_not(odd))
        def _():
            near_relay[q].start()

        far_on[q].start()

    def forward(q):
        near_direct[q].wait_recv()
        near_on[q].start()

    far_apart = jnp.abs(
        lax.broadcasted_iota(jnp.int32, (rows, rows), 0) - lax.broadcasted_iota(jnp.int32, (rows, rows), 1)
    ).astype(jnp.float32)
    for kind in range(KINDS):
        toep[kind], toep_low[kind] = split(jnp.exp(far_apart * (-1.0 / (1 + kind))))
    toeplitz = [(toep[kind], toep_low[kind]) for kind in range(KINDS)]

    start = column_of(starts[pl.ds(half, 1), :].astype(jnp.float32), bands, 0)
    band_ids = lax.broadcasted_iota(jnp.int32, (bands, 1), 0)
    inverse_length = 1.0 / (1.0 + (band_ids % KINDS).astype(jnp.float32))
    channel = lax.broadcasted_iota(jnp.int32, (bands, width), 1).astype(jnp.float32)
    ahead = channel - start
    past = ahead - (window - 1)
    within = jnp.logical_and(ahead >= 0.0, past <= 0.0)
    for kind in range(KINDS):
        windows[kind] = jnp.where(jnp.logical_and(within, band_ids % KINDS == kind), 1.0, 0.0).astype(jnp.bfloat16)
    windows[KINDS] = jnp.where(within, 1.0, 0.0).astype(jnp.bfloat16)
    rise, fall = jnp.exp(-jnp.abs(ahead) * inverse_length), jnp.exp(-jnp.abs(past) * inverse_length)
    ramp[0:bands, :] = jnp.where(within, rise, 0.0)
    ramp[bands:, :] = jnp.where(within, fall, 0.0)
    edge[0:bands, :] = jnp.where(ahead < 0.0, rise, 0.0)
    edge[bands:2 * bands, :] = jnp.where(past > 0.0, fall, 0.0)
    carry_ids = lax.broadcasted_iota(jnp.int32, (2 * KINDS, 1), 0)
    carry_length = 1.0 / (1.0 + (carry_ids % KINDS).astype(jnp.float32))
    carry_channel = lax.broadcasted_iota(jnp.int32, (2 * KINDS, width), 1).astype(jnp.float32) - rows
    upper = carry_ids < KINDS
    carry_gap = jnp.where(upper, carry_channel, -1.0 - carry_channel)
    edge[2 * bands:, :] = jnp.where(carry_gap >= 0.0, jnp.exp(-jnp.abs(carry_gap) * carry_length), 0.0)

    own_split = split(panel[...])
    relay(0)
    for kind in range(KINDS):
        grown[kind] = dot3(toeplitz[kind], own_split, NN)
    relay(1)
    edges = split(edge[...])
    edges_mine, edges_theirs = split(edge[:, mine]), split(edge[:, theirs])
    square, aside = split(panel[:, mine]), split(panel[:, theirs])
    edge_own[:, mine] = dot3(edges_mine, square, NN) + dot3(edges_theirs, aside, NT)
    relay(2)
    edge_own[:, theirs] = dot3(edges_mine, aside, NN)
    relay(3)
    to_turn.wait_recv()
    edge_own[:, theirs] = edge_own[:, theirs] + dot3(edges_theirs, split(turn[...]), NN)
    ramps = split(ramp[...])
    place = lax.broadcasted_iota(jnp.int32, (rows, 1), 0)
    reach_in = jnp.where(first == 0, rows - place, place + 1).astype(jnp.float32)
    for kind in range(KINDS):
        carry = jnp.where(
            first == 0,
            edge_own[2 * bands + kind:2 * bands + kind + 1, :],
            edge_own[2 * bands + KINDS + kind:2 * bands + KINDS + kind + 1, :],
        )
        grown[kind] = grown[kind] + jnp.exp(reach_in * (-1.0 / (1 + kind))) * carry
        felt[kind] = dot3(split(grown[kind]), ramps, NT)
        if kind == 1:
            relay(4)
    own_edges = edge_own[0:2 * bands, :]
    across = dot3(split(own_edges), ramps, NT)
    relay(5)
    middle = CHUNKS // 2
    for q in range(middle):
        forward(q)
    to_sibling.wait_recv()

    def weight(baseline):
        return jnp.sum(jnp.where(partner_row[...] == baseline, 1.0, 0.0), axis=1, keepdims=True)

    pair_near, pair_far = (pair + 1) % pairs * 2, (pair + 2) % pairs * 2
    weights = [
        (sib_own, weight(sibling)), (near, weight(pair_near + core)), (far, weight(pair_far + core)),
        (sib_near, weight(pair_near + 1 - core)), (sib_far, weight(pair_far + 1 - core)),
    ]
    lane = lax.broadcasted_iota(jnp.int32, (1, rows), 1)

    def join(part_index, total, chores):
        span = rows // 2
        low_row = part_index * span
        for q in range(part_index * middle, (part_index + 1) * middle):
            far_on[q].wait_recv()
            near_on[q].wait_recv()
        here = slice(low_row, low_row + span)
        summed = sum(ref[here, :] * factor for ref, factor in weights)
        partners = split(summed)
        columns = pl.ds(pl.multiple_of(first + low_row, span), span)
        ramp_here = split(ramp[:, columns])
        leak = dot3(partners, edges, NT)
        leak_bands = leak[:, 0:2 * bands]
        inner = dot3(ramp_here, split(leak_bands), NN)
        sums = jnp.zeros((KINDS * span, bands), jnp.float32)
        for kind in range(KINDS):
            if kind < len(chores):
                chores[kind]()
            left = dot3((partners[0][:, 0:rows], partners[1][:, 0:rows]), toeplitz[kind], NN)
            left = left + leak[:, 2 * bands + kind:2 * bands + kind + 1] * jnp.exp(
                (rows - lane).astype(jnp.float32) * (-1.0 / (1 + kind)))
            right = dot3((partners[0][:, rows:], partners[1][:, rows:]), toeplitz[kind], NN)
            right = right + leak[:, 2 * bands + KINDS + kind:2 * bands + KINDS + kind + 1] * jnp.exp(
                (lane + 1).astype(jnp.float32) * (-1.0 / (1 + kind)))
            turned = jnp.concatenate([left, right], axis=1)
            pieces = [split(grown[m, here, :] * turned) for m in range(KINDS)]
            stacked = jnp.concatenate([p[0] for p in pieces] + [p[1] for p in pieces], axis=0)
            boxed = dot(stacked, windows[kind], NT)
            sums = sums + (boxed[0:KINDS * span] + boxed[KINDS * span:])
            found = dot3(ramp_here, split(turned), NN)
            crossed[kind] = found if part_index == 0 else crossed[kind] + found
        inside_here = windows[KINDS, :, columns]
        for m in range(KINDS):
            reach = leak_bands * felt[m, here, :]
            high, low = split(sums[m * span:(m + 1) * span] - reach[:, 0:bands] - reach[:, bands:])
            total = total + jnp.where(
                band_ids % KINDS == m, dot(inside_here, high, NN) + dot(inside_here, low, NN), 0.0)
        return inner, total

    inner_0, total = join(0, jnp.zeros((bands, bands), jnp.float32), [
        lambda: relay(6), lambda: relay(7), lambda: forward(4), lambda: forward(5)])
    for q in range(6, CHUNKS):
        forward(q)
    inner_1, total = join(1, total, [])
    cross = (inner_0 + inner_1) * across
    total = total + cross[0:bands, 0:bands] + cross[0:bands, bands:] + cross[bands:, 0:bands] + cross[bands:, bands:]
    side = jnp.zeros((bands, 2 * bands), jnp.float32)
    for kind in range(KINDS):
        high, low = split(crossed[kind] * own_edges)
        side = side + (dot(windows[kind], high, NT) + dot(windows[kind], low, NT))
    eye = (
        lax.broadcasted_iota(jnp.int32, (bands, bands), 0) == lax.broadcasted_iota(jnp.int32, (bands, bands), 1)
    ).astype(jnp.float32)
    flipped = exact(eye, total, NT) - side[:, 0:bands] - side[:, bands:]
    flipped = flipped * (1.0 / (4 * groups * window))

    everyone = groups * owners
    span = tile_rows * band_share
    lanes = owners * span
    source = lax.broadcasted_iota(jnp.int32, (bands, lanes), 0)
    lane_ids = lax.broadcasted_iota(jnp.int32, (bands, lanes), 1)
    wanted = lane_ids // span * band_share + lane_ids % band_share
    repeated = exact(flipped, (source == wanted).astype(jnp.float32), NN)
    kept = jnp.where(source % tile_rows == lane_ids % span // band_share, repeated, 0.0)
    gather = lax.broadcasted_iota(jnp.int32, (groups, bands), 1) // tile_rows == lax.broadcasted_iota(
        jnp.int32, (groups, bands), 0)
    packed = exact(gather.astype(jnp.float32), kept, NN)
    for z in range(owners):
        for g in range(groups):
            tiles[z * groups + g] = packed[g:g + 1, z * span:(z + 1) * span]
    here = level * groups + me
    landed[pl.ds(here, 1)] = tiles[pl.ds(here, 1)]
    pl.semaphore_wait(ready, groups - 1)
    outgoing = []
    for d in range(1, everyone):
        peer = (here + d) % everyone
        copy = pltpu.make_async_remote_copy(
            src_ref=tiles.at[peer], dst_ref=landed.at[here], send_sem=fin_send.at[peer], recv_sem=fin_recv.at[here],
            device_id=(peer % groups, peer // groups), device_id_type=MESH,
        )
        copy.start()
        outgoing.append(copy)
    for d in range(1, everyone):
        peer = (here + d) % everyone
        pltpu.make_async_remote_copy(
            src_ref=tiles.at[peer], dst_ref=landed.at[peer], send_sem=fin_send.at[peer], recv_sem=fin_recv.at[peer],
            device_id=(peer % groups, peer // groups), device_id_type=MESH,
        ).wait_recv()
    row_ids = lax.broadcasted_iota(jnp.int32, (tile_rows, span), 0)
    keep = row_ids == lax.broadcasted_iota(jnp.int32, (tile_rows, span), 1) // band_share
    pick = lax.broadcasted_iota(jnp.int32, (span, band_share), 0) % band_share == lax.broadcasted_iota(
        jnp.int32, (span, band_share), 1)
    for h in range(2):
        row = jnp.sum(landed[h * everyone // 2:(h + 1) * everyone // 2], axis=0)
        out_ref[h] = exact(jnp.where(keep, row, 0.0), pick.astype(jnp.float32), NN)

    for copy in outgoing:
        copy.wait_send()
    for q in range(CHUNKS):
        to_far[q].wait_send()
        near_direct[q].wait_send()
        far_on[q].wait_send()
        near_on[q].wait_send()
    to_sibling.wait_send()
    to_turn.wait_send()


def solution(mesh):
    groups, owners = mesh.shape["bl"], mesh.shape["bp"]

    def body(inverse_cov, channel_keep_mask, partner_ids, band_starts):
        count, rows, channels = inverse_cov.shape
        width, bands = channels // 2, band_starts.shape[1]
        assert count == 1 and groups % 4 == 0 and width == 2 * rows
        f32, bf16 = jnp.float32, jnp.bfloat16
        block = pltpu.VMEM((rows, width), f32)
        tile_rows = bands // groups
        dma = pltpu.SemaphoreType.DMA
        vmem = pl.BlockSpec(memory_space=pltpu.VMEM)
        found = pl.pallas_call(
            partial(kernel, (groups, owners, rows, width, bands)),
            name="fisher",
            out_shape=jax.ShapeDtypeStruct((2, tile_rows, bands // owners), f32),
            in_specs=[pl.BlockSpec(memory_space=pltpu.HBM)] * 4,
            out_specs=vmem,
            scratch_shapes=[
                block,
                pltpu.VMEM(channel_keep_mask.shape, jnp.int32),
                pltpu.VMEM(partner_ids.shape, jnp.int32),
                pltpu.VMEM(band_starts.shape, jnp.int32),
                block,
                pltpu.VMEM((rows, rows), f32),
                block, block, block, block, block,
                pltpu.VMEM((KINDS, rows, rows), bf16),
                pltpu.VMEM((KINDS, rows, rows), bf16),
                pltpu.VMEM((KINDS, rows, width), f32),
                pltpu.VMEM((KINDS, rows, 2 * bands), f32),
                pltpu.VMEM((KINDS + 1, bands, width), bf16),
                pltpu.VMEM((2 * bands, width), f32),
                pltpu.VMEM((2 * bands + 2 * KINDS, width), f32),
                pltpu.VMEM((2 * bands + 2 * KINDS, width), f32),
                pltpu.VMEM((KINDS, 2 * bands, width), f32),
                pltpu.VMEM((groups * owners, 1, tile_rows * bands // owners), f32),
                pltpu.VMEM((groups * owners, 1, tile_rows * bands // owners), f32),
                dma((4,)), dma((2, 1)), dma((2, 1)),
                dma((2, CHUNKS)), dma((2, CHUNKS)), dma((2, CHUNKS)), dma((2, CHUNKS)),
                dma((groups * owners,)), dma((groups * owners,)), pltpu.SemaphoreType.REGULAR,
            ],
            compiler_params=pltpu.CompilerParams(
                collective_id=0, has_side_effects=True, vmem_limit_bytes=67043328
            ),
        )(inverse_cov, channel_keep_mask, partner_ids, band_starts)
        return jnp.swapaxes(found, 1, 2)

    placed = (P("bl", "bp", None), P("bl", None), P("bl", None), P())
    return jax.shard_map(body, mesh=mesh, in_specs=placed, out_specs=P(None, "bp", "bl"), check_vma=False)
```

```python
from functools import partial

import jax
import jax.numpy as jnp
from jax import lax
from jax.experimental import pallas as pl
from jax.experimental.pallas import tpu as pltpu
from jax.sharding import PartitionSpec as P

WINDOW_LENGTH = 128
KINDS = 4
CHUNKS = 8
PARTS = ((0, 4), (4, 8))
MESH = pl.DeviceIdType.MESH
NT = (((1,), (1,)), ((), ()))
NN = (((1,), (0,)), ((), ()))


def split(value):
    high = value.astype(jnp.bfloat16)
    return high, (value - high.astype(jnp.float32)).astype(jnp.bfloat16)


def dot(left, right, dims):
    return lax.dot_general(left, right, dims, preferred_element_type=jnp.float32)


def dot3(left, right, dims):
    return dot(left[0], right[0], dims) + (dot(left[0], right[1], dims) + dot(left[1], right[0], dims))


def exact(left, right, dims):
    return lax.dot_general(
        left, right, dims, precision=lax.Precision.HIGHEST, preferred_element_type=jnp.float32
    )


def column_of(row, length, offset):
    shape = (length, row.shape[1])
    spot = lax.broadcasted_iota(jnp.int32, shape, 0) + offset == lax.broadcasted_iota(jnp.int32, shape, 1)
    return jnp.sum(jnp.where(spot, row, 0.0), axis=1, keepdims=True)


def kernel(
    sizes, cov_ref, mask_ref, partner_ref, starts_ref, out_ref,
    raw, masks, partner_row, starts, panel, turn, near, far, sib_own, sib_near, sib_far, toep, toep_low, grown, felt,
    windows, ramp, edge, edge_own, crossed, tiles, landed,
    load_sem, sib_sem, turn_sem, far_sem, near_sem, sfar_sem, snear_sem, fin_send, fin_recv, ready,
):
    groups, owners, rows, width, bands = sizes
    window = WINDOW_LENGTH
    me, level = lax.axis_index("bl"), lax.axis_index("bp")
    per_half = width // rows
    half, first = level // per_half, pl.multiple_of(level % per_half * rows, rows)
    pair, core = me // 2, me % 2
    pairs = groups // 2
    sibling = pair * 2 + 1 - core
    beside = (pair + 1 - 2 * (pair % 2)) * 2 + core
    behind = (pair + pairs - 2) % pairs * 2 + core
    level_other = level // per_half * per_half + (per_half - 1 - level % per_half)
    tile_rows = bands // groups
    band_share = bands // owners
    step = rows // CHUNKS

    half_columns = pl.ds(pl.multiple_of(half * width, width), width)
    loads = [
        pltpu.make_async_copy(source, target, load_sem.at[index])
        for index, (source, target) in enumerate([
            (cov_ref.at[0, :, half_columns], raw),
            (mask_ref, masks),
            (starts_ref, starts),
            (partner_ref, partner_row),
        ])
    ]
    for load in loads:
        load.start()
    barrier = pltpu.get_barrier_semaphore()
    for d in range(1, groups):
        pl.semaphore_signal(barrier, inc=1, device_id=((me + d) % groups, level), device_id_type=MESH)
    for d in range(1, owners):
        pl.semaphore_signal(barrier, inc=1, device_id=(me, (level + d) % owners), device_id_type=MESH)
    for load in loads:
        load.wait()

    marks = masks[:, half_columns].astype(jnp.float32)
    row_marks = column_of(marks, rows, first)
    panel[...] = raw[...] * row_marks * marks
    pl.semaphore_wait(barrier, groups + owners - 2)

    def remote(source, target, sems, index, device):
        return pltpu.make_async_remote_copy(
            src_ref=source, dst_ref=target, send_sem=sems.at[0, index], recv_sem=sems.at[1, index],
            device_id=device, device_id_type=MESH,
        )

    def own_at(q):
        return panel.at[pl.ds(q * step, step)]

    def part(ref, q):
        return ref.at[pl.ds(q * step, step)]

    to_far = [remote(own_at(q), part(far, q), far_sem, q, (behind, level)) for q in range(CHUNKS)]
    near_direct = [remote(own_at(q), part(near, q), near_sem, q, (beside, level)) for q in range(CHUNKS)]
    near_relay = [remote(part(far, q), part(near, q), near_sem, q, (beside, level)) for q in range(CHUNKS)]
    far_on = [remote(part(far, q), part(sib_far, q), sfar_sem, q, (sibling, level)) for q in range(CHUNKS)]
    near_on = [remote(part(near, q), part(sib_near, q), snear_sem, q, (sibling, level)) for q in range(CHUNKS)]
    mine = pl.ds(first, rows)
    theirs = pl.ds(pl.multiple_of(width - rows - first, rows), rows)
    to_sibling = remote(panel, sib_own, sib_sem, 0, (sibling, level))
    to_turn = remote(panel.at[:, mine], turn, turn_sem, 0, (me, level_other))

    odd = pair % 2 == 1
    for q in range(CHUNKS):
        to_far[q].start()

        @pl.when(odd)
        def _():
            near_direct[q].start()

    to_turn.start()
    to_sibling.start()
    for d in range(1, groups):
        pl.semaphore_signal(ready, inc=1, device_id=((me + d) % groups, level), device_id_type=MESH)

    def relay(q):
        to_far[q].wait_recv()

        @pl.when(jnp.logical_not(odd))
        def _():
            near_relay[q].start()

        far_on[q].start()

    def forward(q):
        near_direct[q].wait_recv()
        near_on[q].start()

    far_apart = jnp.abs(
        lax.broadcasted_iota(jnp.int32, (rows, rows), 0) - lax.broadcasted_iota(jnp.int32, (rows, rows), 1)
    ).astype(jnp.float32)
    for kind in range(KINDS):
        toep[kind], toep_low[kind] = split(jnp.exp(far_apart * (-1.0 / (1 + kind))))
    toeplitz = [(toep[kind], toep_low[kind]) for kind in range(KINDS)]

    start = column_of(starts[pl.ds(half, 1), :].astype(jnp.float32), bands, 0)
    band_ids = lax.broadcasted_iota(jnp.int32, (bands, 1), 0)
    inverse_length = 1.0 / (1.0 + (band_ids % KINDS).astype(jnp.float32))
    channel = lax.broadcasted_iota(jnp.int32, (bands, width), 1).astype(jnp.float32)
    ahead = channel - start
    past = ahead - (window - 1)
    within = jnp.logical_and(ahead >= 0.0, past <= 0.0)
    for kind in range(KINDS):
        windows[kind] = jnp.where(jnp.logical_and(within, band_ids % KINDS == kind), 1.0, 0.0).astype(jnp.bfloat16)
    windows[KINDS] = jnp.where(within, 1.0, 0.0).astype(jnp.bfloat16)
    rise, fall = jnp.exp(-jnp.abs(ahead) * inverse_length), jnp.exp(-jnp.abs(past) * inverse_length)
    ramp[0:bands, :] = jnp.where(within, rise, 0.0)
    ramp[bands:, :] = jnp.where(within, fall, 0.0)
    edge[0:bands, :] = jnp.where(ahead < 0.0, rise, 0.0)
    edge[bands:2 * bands, :] = jnp.where(past > 0.0, fall, 0.0)
    carry_ids = lax.broadcasted_iota(jnp.int32, (2 * KINDS, 1), 0)
    carry_length = 1.0 / (1.0 + (carry_ids % KINDS).astype(jnp.float32))
    carry_channel = lax.broadcasted_iota(jnp.int32, (2 * KINDS, width), 1).astype(jnp.float32) - rows
    upper = carry_ids < KINDS
    carry_gap = jnp.where(upper, carry_channel, -1.0 - carry_channel)
    edge[2 * bands:, :] = jnp.where(carry_gap >= 0.0, jnp.exp(-jnp.abs(carry_gap) * carry_length), 0.0)

    own_split = split(panel[...])
    relay(0)
    for kind in range(KINDS):
        grown[kind] = dot3(toeplitz[kind], own_split, NN)
    relay(1)
    edges = split(edge[...])
    edges_mine, edges_theirs = split(edge[:, mine]), split(edge[:, theirs])
    square, aside = split(panel[:, mine]), split(panel[:, theirs])
    edge_own[:, mine] = dot3(edges_mine, square, NN) + dot3(edges_theirs, aside, NT)
    relay(2)
    edge_own[:, theirs] = dot3(edges_mine, aside, NN)
    relay(3)
    to_turn.wait_recv()
    edge_own[:, theirs] = edge_own[:, theirs] + dot3(edges_theirs, split(turn[...]), NN)
    ramps = split(ramp[...])
    place = lax.broadcasted_iota(jnp.int32, (rows, 1), 0)
    reach_in = jnp.where(first == 0, rows - place, place + 1).astype(jnp.float32)
    for kind in range(KINDS):
        carry = jnp.where(
            first == 0,
            edge_own[2 * bands + kind:2 * bands + kind + 1, :],
            edge_own[2 * bands + KINDS + kind:2 * bands + KINDS + kind + 1, :],
        )
        grown[kind] = grown[kind] + jnp.exp(reach_in * (-1.0 / (1 + kind))) * carry
        felt[kind] = dot3(split(grown[kind]), ramps, NT)
        if kind == 1:
            relay(4)
    own_edges = edge_own[0:2 * bands, :]
    across = dot3(split(own_edges), ramps, NT)
    relay(5)
    for q in range(PARTS[0][1]):
        forward(q)
    relay(6)
    to_sibling.wait_recv()

    def weight(baseline):
        return jnp.sum(jnp.where(partner_row[...] == baseline, 1.0, 0.0), axis=1, keepdims=True)

    pair_near, pair_far = (pair + 1) % pairs * 2, (pair + 2) % pairs * 2
    weights = [
        (sib_own, weight(sibling)), (near, weight(pair_near + core)), (far, weight(pair_far + core)),
        (sib_near, weight(pair_near + 1 - core)), (sib_far, weight(pair_far + 1 - core)),
    ]
    lane = lax.broadcasted_iota(jnp.int32, (1, rows), 1)

    def join(part_index, total, chores):
        begin, end = PARTS[part_index]
        span, low_row = (end - begin) * step, begin * step
        for q in range(begin, end):
            far_on[q].wait_recv()
            near_on[q].wait_recv()
        here = slice(low_row, low_row + span)
        summed = sum(ref[here, :] * factor for ref, factor in weights)
        partners = split(summed)
        ramp_here = split(ramp[:, mine][:, here])
        leak = dot3(partners, edges, NT)
        leak_bands = leak[:, 0:2 * bands]
        inner = dot3(ramp_here, split(leak_bands), NN)
        sums = jnp.zeros((KINDS * span, bands), jnp.float32)
        for kind in range(KINDS):
            if kind < len(chores):
                chores[kind]()
            left = dot3((partners[0][:, 0:rows], partners[1][:, 0:rows]), toeplitz[kind], NN)
            left = left + leak[:, 2 * bands + kind:2 * bands + kind + 1] * jnp.exp(
                (rows - lane).astype(jnp.float32) * (-1.0 / (1 + kind)))
            right = dot3((partners[0][:, rows:], partners[1][:, rows:]), toeplitz[kind], NN)
            right = right + leak[:, 2 * bands + KINDS + kind:2 * bands + KINDS + kind + 1] * jnp.exp(
                (lane + 1).astype(jnp.float32) * (-1.0 / (1 + kind)))
            turned = jnp.concatenate([left, right], axis=1)
            pieces = [split(grown[m, here, :] * turned) for m in range(KINDS)]
            stacked = jnp.concatenate([p[0] for p in pieces] + [p[1] for p in pieces], axis=0)
            boxed = dot(stacked, windows[kind], NT)
            sums = sums + (boxed[0:KINDS * span] + boxed[KINDS * span:])
            found = dot3(ramp_here, split(turned), NN)
            crossed[kind] = found if part_index == 0 else crossed[kind] + found
        inside_here = windows[KINDS, :, mine][:, here]
        for m in range(KINDS):
            reach = leak_bands * felt[m, here, :]
            high, low = split(sums[m * span:(m + 1) * span] - reach[:, 0:bands] - reach[:, bands:])
            total = total + jnp.where(
                band_ids % KINDS == m, dot(inside_here, high, NN) + dot(inside_here, low, NN), 0.0)
        return inner, total

    done, relayed = PARTS[0][1], 7
    inner, total = 0.0, jnp.zeros((bands, bands), jnp.float32)
    for part_index in range(len(PARTS)):
        chores = []
        if part_index + 1 < len(PARTS):
            chores = [partial(relay, q) for q in range(relayed, CHUNKS)]
            chores += [partial(forward, q) for q in range(done, PARTS[part_index + 1][1])]
            relayed, done = CHUNKS, PARTS[part_index + 1][1]
        found, total = join(part_index, total, chores[:KINDS])
        inner = inner + found
        for chore in chores[KINDS:]:
            chore()
    cross = inner * across
    total = total + cross[0:bands, 0:bands] + cross[0:bands, bands:] + cross[bands:, 0:bands] + cross[bands:, bands:]
    side = jnp.zeros((bands, 2 * bands), jnp.float32)
    for kind in range(KINDS):
        high, low = split(crossed[kind] * own_edges)
        side = side + (dot(windows[kind], high, NT) + dot(windows[kind], low, NT))
    eye = (
        lax.broadcasted_iota(jnp.int32, (bands, bands), 0) == lax.broadcasted_iota(jnp.int32, (bands, bands), 1)
    ).astype(jnp.float32)
    flipped = exact(eye, total, NT) - side[:, 0:bands] - side[:, bands:]
    flipped = flipped * (1.0 / (4 * groups * window))

    everyone = groups * owners
    span = tile_rows * band_share
    lanes = owners * span
    source = lax.broadcasted_iota(jnp.int32, (bands, lanes), 0)
    lane_ids = lax.broadcasted_iota(jnp.int32, (bands, lanes), 1)
    wanted = lane_ids // span * band_share + lane_ids % band_share
    repeated = exact(flipped, (source == wanted).astype(jnp.float32), NN)
    kept = jnp.where(source % tile_rows == lane_ids % span // band_share, repeated, 0.0)
    gather = lax.broadcasted_iota(jnp.int32, (groups, bands), 1) // tile_rows == lax.broadcasted_iota(
        jnp.int32, (groups, bands), 0)
    packed = exact(gather.astype(jnp.float32), kept, NN)
    for z in range(owners):
        for g in range(groups):
            tiles[z * groups + g] = packed[g:g + 1, z * span:(z + 1) * span]
    here = level * groups + me
    landed[pl.ds(here, 1)] = tiles[pl.ds(here, 1)]
    pl.semaphore_wait(ready, groups - 1)
    outgoing = []
    for d in range(1, everyone):
        peer = (here + d) % everyone
        copy = pltpu.make_async_remote_copy(
            src_ref=tiles.at[peer], dst_ref=landed.at[here], send_sem=fin_send.at[peer], recv_sem=fin_recv.at[here],
            device_id=(peer % groups, peer // groups), device_id_type=MESH,
        )
        copy.start()
        outgoing.append(copy)
    for d in range(1, everyone):
        peer = (here + d) % everyone
        pltpu.make_async_remote_copy(
            src_ref=tiles.at[peer], dst_ref=landed.at[peer], send_sem=fin_send.at[peer], recv_sem=fin_recv.at[peer],
            device_id=(peer % groups, peer // groups), device_id_type=MESH,
        ).wait_recv()
    row_ids = lax.broadcasted_iota(jnp.int32, (tile_rows, span), 0)
    keep = row_ids == lax.broadcasted_iota(jnp.int32, (tile_rows, span), 1) // band_share
    pick = lax.broadcasted_iota(jnp.int32, (span, band_share), 0) % band_share == lax.broadcasted_iota(
        jnp.int32, (span, band_share), 1)
    for h in range(2):
        row = jnp.sum(landed[h * everyone // 2:(h + 1) * everyone // 2], axis=0)
        out_ref[h] = exact(jnp.where(keep, row, 0.0), pick.astype(jnp.float32), NN)

    for copy in outgoing:
        copy.wait_send()
    for q in range(CHUNKS):
        to_far[q].wait_send()
        near_direct[q].wait_send()
        far_on[q].wait_send()
        near_on[q].wait_send()
    to_sibling.wait_send()
    to_turn.wait_send()


def solution(mesh):
    groups, owners = mesh.shape["bl"], mesh.shape["bp"]

    def body(inverse_cov, channel_keep_mask, partner_ids, band_starts):
        count, rows, channels = inverse_cov.shape
        width, bands = channels // 2, band_starts.shape[1]
        assert count == 1 and groups % 4 == 0 and width == 2 * rows
        f32, bf16 = jnp.float32, jnp.bfloat16
        block = pltpu.VMEM((rows, width), f32)
        tile_rows = bands // groups
        dma = pltpu.SemaphoreType.DMA
        vmem = pl.BlockSpec(memory_space=pltpu.VMEM)
        found = pl.pallas_call(
            partial(kernel, (groups, owners, rows, width, bands)),
            name="fisher",
            out_shape=jax.ShapeDtypeStruct((2, tile_rows, bands // owners), f32),
            in_specs=[pl.BlockSpec(memory_space=pltpu.HBM)] * 4,
            out_specs=vmem,
            scratch_shapes=[
                block,
                pltpu.VMEM(channel_keep_mask.shape, jnp.int32),
                pltpu.VMEM(partner_ids.shape, jnp.int32),
                pltpu.VMEM(band_starts.shape, jnp.int32),
                block,
                pltpu.VMEM((rows, rows), f32),
                block, block, block, block, block,
                pltpu.VMEM((KINDS, rows, rows), bf16),
                pltpu.VMEM((KINDS, rows, rows), bf16),
                pltpu.VMEM((KINDS, rows, width), f32),
                pltpu.VMEM((KINDS, rows, 2 * bands), f32),
                pltpu.VMEM((KINDS + 1, bands, width), bf16),
                pltpu.VMEM((2 * bands, width), f32),
                pltpu.VMEM((2 * bands + 2 * KINDS, width), f32),
                pltpu.VMEM((2 * bands + 2 * KINDS, width), f32),
                pltpu.VMEM((KINDS, 2 * bands, width), f32),
                pltpu.VMEM((groups * owners, 1, tile_rows * bands // owners), f32),
                pltpu.VMEM((groups * owners, 1, tile_rows * bands // owners), f32),
                dma((4,)), dma((2, 1)), dma((2, 1)),
                dma((2, CHUNKS)), dma((2, CHUNKS)), dma((2, CHUNKS)), dma((2, CHUNKS)),
                dma((groups * owners,)), dma((groups * owners,)), pltpu.SemaphoreType.REGULAR,
            ],
            compiler_params=pltpu.CompilerParams(
                collective_id=0, has_side_effects=True, vmem_limit_bytes=67043328
            ),
        )(inverse_cov, channel_keep_mask, partner_ids, band_starts)
        return jnp.swapaxes(found, 1, 2)

    placed = (P("bl", "bp", None), P("bl", None), P("bl", None), P())
    return jax.shard_map(body, mesh=mesh, in_specs=placed, out_specs=P(None, "bp", "bl"), check_vma=False)
```
